512 devices in a mesh: grp: 16 (over y, core), blk: 32 (over z, x).
Axes of the slice: x: 4, y: 8, z: 8, core: 2. Of those that a mesh axis runs over, the one named last changes fastest.
Arguments:
- queries: bfloat16 [16, 512, 4096], P(None, ('blk', 'grp')), may hold values from -24 to 24
- cache_keys: bfloat16 [16, 14336, 512], P('grp', 'blk'), may hold values from -24 to 24
- cache_values: bfloat16 [16, 14336, 512], P('grp', 'blk'), may hold values from -15 to 15
- new_keys: bfloat16 [16, 512, 512], P(None, ('blk', 'grp')), may hold values from -6 to 6
- new_values: bfloat16 [16, 512, 512], P(None, ('blk', 'grp')), may hold values from -15 to 15
- hits: int32 [16], P('grp'), may hold values from 1792 to 14336, as said below
- counts: int32 [16], P('grp'), may hold values from 256 to 512, as said below
- assign: int32 [16, 32], P('grp'), may hold values from 0 to 31, each once within a row
Outputs:
- attended: bfloat16 [16, 512, 4096], P(None, ('blk', 'grp'))
The draws below stay inside these ranges and needn't reach their ends.
Inputs may be any that keep to these rules, and one draw needn't show every extreme that they name: Cached positions of request r below hits[r] are valid; in every draw some request has all 14336 valid. New tokens of request r at order counts[r] or later are padding; in every draw some request has all 512.
All inputs are finite; a program needn't handle non-finite values.
Results may differ from the reference program's by a relative error of at most 0.0085.
Values may be sent and summed in bfloat16 or wider, within the bound.
A program may use at most 128 MiB of HBM per device.

```python
import jax
import jax.numpy as jnp
from jax import lax

HEADS = 32
KV_HEADS = 4
HEAD_DIM = 128
Q_DEV = 16
C_DEV = 448
REQ = 16
NEW = 512
CTX = 14336
N_BLK = 32


def shared_keys(key):
    return jnp.clip(jax.random.normal(jax.random.fold_in(key, 11), (REQ, CTX, KV_HEADS * HEAD_DIM), jnp.float32), -5.0, 5.0)


def draw_cache_keys(key, part):
    keys = shared_keys(key)
    return keys.astype(jnp.bfloat16)


def draw_queries(key, part):
    base = 2.0 * jnp.clip(jax.random.normal(jax.random.fold_in(key, 12), (REQ, NEW, HEADS * HEAD_DIM), jnp.float32), -5.0, 5.0)
    return base.astype(jnp.bfloat16)


def draw_hits(key, part):
    values = jax.random.randint(jax.random.fold_in(key, 21), (REQ,), CTX // 8, CTX + 1, jnp.int32)
    chosen = jax.random.randint(jax.random.fold_in(key, 22), (), 0, REQ, jnp.int32)
    return values.at[chosen].set(CTX)


def draw_counts(key, part):
    values = jax.random.randint(jax.random.fold_in(key, 31), (REQ,), NEW // 2, NEW + 1, jnp.int32)
    chosen = jax.random.randint(jax.random.fold_in(key, 32), (), 0, REQ, jnp.int32)
    return values.at[chosen].set(NEW)


def level_of(own_key, dims, pieces, low, largest):
    def one(dim, blocks):
        heights = jax.random.uniform(jax.random.fold_in(jax.random.fold_in(own_key, 6), dim), (blocks,), jnp.float32, low / len(pieces), largest / len(pieces))
        return jnp.repeat(jnp.exp(heights), dims[dim] // blocks).reshape((-1,) + (1,) * (len(dims) - dim - 1))

    gain = one(*pieces[0])
    for cut in pieces[1:]:
        gain = gain * one(*cut)
    return gain


def normal_values(key, extent, scale, most, cuts=(), kind=jnp.bfloat16):
    array = jax.random.normal(key, extent, jnp.float32) * scale
    if len(cuts) > 0:
        array = level_of(key, extent, cuts, -0.22, 0.18) * array
    return jnp.clip(array, min=-most, max=most).astype(kind)


def setup_inputs(seed: int = 0) -> dict:
    key_of = jax.random.split(jax.random.key(seed), 9)
    return {
        "queries": draw_queries(jax.random.fold_in(key_of[8], 71), 0),
        "cache_keys": draw_cache_keys(jax.random.fold_in(key_of[8], 71), 0),
        "cache_values": normal_values(key_of[2], (REQ, CTX, KV_HEADS * HEAD_DIM), 3.0, 15.0, ((0, 16), (1, 32))),
        "new_keys": normal_values(key_of[3], (REQ, NEW, KV_HEADS * HEAD_DIM), 1.0, 6.0, ((1, 512),)),
        "new_values": normal_values(key_of[4], (REQ, NEW, KV_HEADS * HEAD_DIM), 3.0, 15.0, ((1, 512),)),
        "hits": draw_hits(jax.random.fold_in(key_of[8], 71), 0),
        "counts": draw_counts(jax.random.fold_in(key_of[8], 71), 0),
        "assign": jax.vmap(lambda own: jax.random.permutation(own, N_BLK))(jax.random.split(key_of[7], REQ)).reshape((REQ, N_BLK)).astype(jnp.int32),
    }


def partial_block(queries, keys, values, allowed, kv_heads):
    row_count, full_width = queries.shape
    key_count = keys.shape[0]
    head_dim = keys.shape[1] // kv_heads
    group_size = full_width // head_dim // kv_heads
    query_heads = queries.astype(jnp.float32).reshape(row_count, kv_heads, group_size, head_dim)
    key_heads = keys.astype(jnp.float32).reshape(key_count, kv_heads, head_dim)
    scores = jnp.einsum("qkgd,nkd->kgqn", query_heads, key_heads) * (head_dim ** -0.5)
    scores = jnp.where(allowed[None, None], scores, -1e30)
    block_max = jnp.max(scores, axis=-1)
    exp_terms = jnp.where(allowed[None, None], jnp.exp(scores - block_max[..., None]), 0.0)
    weight_sum = jnp.sum(exp_terms, axis=-1)
    prob_bf = lax.optimization_barrier(exp_terms.astype(jnp.bfloat16)).astype(jnp.float32)
    value_heads = values.astype(jnp.float32).reshape(key_count, kv_heads, head_dim)
    blended = jnp.einsum("kgqn,nkd->qkgd", prob_bf, value_heads)
    floor_sum = jnp.maximum(weight_sum, 1.0).transpose(2, 0, 1)[..., None]
    blended = (blended / floor_sum).reshape(row_count, full_width).astype(jnp.bfloat16)
    maxima = block_max.transpose(2, 0, 1).reshape(row_count, -1)
    weights = weight_sum.transpose(2, 0, 1).reshape(row_count, -1)
    return blended, maxima, weights


def combine(running, part, head_count):
    summed, maxima, weights = running
    blended, part_max, part_weight = part
    row_count, full_width = summed.shape
    highest = jnp.maximum(maxima, part_max)
    old_scale = jnp.exp(maxima - highest)
    new_scale = part_weight * jnp.exp(part_max - highest)
    summed = summed.reshape(row_count, head_count, -1) * old_scale[:, :, None]
    summed = summed + new_scale[:, :, None] * blended.astype(jnp.float32).reshape(row_count, head_count, -1)
    return summed.reshape(row_count, full_width), highest, weights * old_scale + new_scale


def one_request(items):
    query_rows, cache_k, cache_v, fresh_k, fresh_v, hit_limit, filled, block_order = items
    full_width = query_rows.shape[1]
    head_count = full_width // HEAD_DIM
    kv_heads = fresh_k.shape[1] // HEAD_DIM
    lanes = jnp.arange(NEW, dtype=jnp.int32)
    query_pos = block_order[lanes // Q_DEV] * Q_DEV + lanes % Q_DEV
    cache_lane = jnp.arange(C_DEV, dtype=jnp.int32)
    fresh_lane = jnp.arange(Q_DEV, dtype=jnp.int32)
    start = (jnp.zeros((NEW, full_width), jnp.float32), jnp.full((NEW, head_count), -1e30, jnp.float32), jnp.zeros((NEW, head_count), jnp.float32))

    def add_block(running, block_index):
        cache_first = (block_index * C_DEV).astype(jnp.int32)
        fresh_first = (block_index * Q_DEV).astype(jnp.int32)
        keys_here = jnp.concatenate([lax.dynamic_slice_in_dim(cache_k, cache_first, C_DEV, 0), lax.dynamic_slice_in_dim(fresh_k, fresh_first, Q_DEV, 0)], 0)
        values_here = jnp.concatenate([lax.dynamic_slice_in_dim(cache_v, cache_first, C_DEV, 0), lax.dynamic_slice_in_dim(fresh_v, fresh_first, Q_DEV, 0)], 0)
        cache_ok = (block_index * C_DEV + cache_lane) < hit_limit
        fresh_ok = (block_order[block_index] * Q_DEV + fresh_lane)[None, :] <= query_pos[:, None]
        allowed = jnp.concatenate([jnp.broadcast_to(cache_ok[None, :], (NEW, C_DEV)), fresh_ok], 1)
        part = partial_block(query_rows, keys_here, values_here, allowed, kv_heads)
        return combine(running, part, head_count), None

    running, _ = lax.scan(add_block, start, jnp.arange(N_BLK, dtype=jnp.int32))
    summed, maxima, weights = running
    blended = (summed.reshape(NEW, head_count, -1) / weights[:, :, None]).reshape(NEW, full_width)
    blended = jnp.where((query_pos < filled)[:, None], blended, 0.0)
    return blended.astype(jnp.bfloat16)


def reference(queries, cache_keys, cache_values, new_keys, new_values, hits, counts, assign):
    return lax.map(one_request, (queries, cache_keys, cache_values, new_keys, new_values, hits, counts, assign))
```

```python
import functools

import jax
import jax.numpy as jnp
from jax import lax
from jax.experimental import pallas as pl
from jax.experimental.pallas import tpu as pltpu
from jax.sharding import Mesh
from jax.sharding import PartitionSpec as P

HEAD_DIM = 128
GROUP = 8
BLK = ("blk_0", "blk_1")
BLK_GRP = ("blk_0", "blk_1", "grp")
NEG = -1e30
TO_LOG2 = HEAD_DIM**-0.5 * 1.4426950408889634


def kernel(
    G, NZ, NX, C,
    q_in, kv_in, ck, cv, hits, counts, assign,
    out,
    qy, kvy, Q, K, VA, kvn, KN, VN, bias, OP, LP, OR, LR, W, res, OX,
    loc, ys, yr, xs, xr, cs, cr, ags, agr, os_, or_, fs, fr, ts, tr,
):
    g, z, x = lax.axis_index("grp"), lax.axis_index("blk_0"), lax.axis_index("blk_1")
    T = NX * G
    GR = G * GROUP
    H = NZ // 2
    PN = KN.shape[0]

    def remote(src, dst, ssem, rsem, **where):
        return pltpu.make_async_remote_copy(
            src_ref=src, dst_ref=dst, send_sem=ssem, recv_sem=rsem,
            device_id=where, device_id_type=pl.DeviceIdType.MESH,
        )

    def each(n, fn):
        def body(i, carry):
            fn(i)
            return carry
        lax.fori_loop(1, n, body, 0)

    barrier = pltpu.get_barrier_semaphore()

    def greet(axis, me, n):
        each(n, lambda i: pl.semaphore_signal(
            barrier, 1, device_id={axis: lax.rem(me + i, n)},
            device_id_type=pl.DeviceIdType.MESH))

    greet("grp", g, G)
    greet("blk_1", x, NX)
    greet("blk_0", z, NZ)

    own_lane = pl.ds(pl.multiple_of(x * HEAD_DIM, HEAD_DIM), HEAD_DIM)
    own_rows = pl.ds(pl.multiple_of(x * C, C), C)
    l_q = pltpu.make_async_copy(q_in.at[g], qy.at[g], loc.at[0])
    l_kv = pltpu.make_async_copy(kv_in.at[g], kvy.at[g], loc.at[1])
    l_k = pltpu.make_async_copy(ck.at[:, own_lane], K.at[own_rows], loc.at[2])
    l_v = pltpu.make_async_copy(cv.at[:, own_lane], VA.at[own_rows, pl.ds(0, HEAD_DIM)], loc.at[3])
    for c in (l_q, l_kv, l_k, l_v):
        c.start()

    VA[:, HEAD_DIM:] = jnp.ones((NX * C, HEAD_DIM), jnp.bfloat16)
    KN[...] = jnp.zeros((PN, HEAD_DIM), jnp.bfloat16)
    VN[:, :HEAD_DIM] = jnp.zeros((PN, HEAD_DIM), jnp.bfloat16)
    VN[:, HEAD_DIM:] = jnp.ones((PN, HEAD_DIM), jnp.bfloat16)
    limit = hits[0] - z * (NX * C)
    col = lax.broadcasted_iota(jnp.int32, (1, NX * C), 1)
    bias[...] = jnp.where(col < limit, 0.0, NEG).astype(jnp.float32)

    pl.semaphore_wait(barrier, (G - 1) + (NX - 1) + (NZ - 1))

    def y_q(i):
        p = lax.rem(g + i, G)
        return remote(q_in.at[p], qy.at[g], ys.at[0, p], yr.at[0, g], grp=p)

    def y_kv(i):
        p = lax.rem(g + i, G)
        return remote(kv_in.at[p], kvy.at[g], ys.at[1, p], yr.at[1, g], grp=p)

    each(G, lambda i: y_q(i).start())
    each(G, lambda i: y_kv(i).start())

    def x_k(i):
        p = lax.rem(x + i, NX)
        lane = pl.ds(pl.multiple_of(p * HEAD_DIM, HEAD_DIM), HEAD_DIM)
        return remote(ck.at[:, lane], K.at[own_rows], cs.at[0, p], cr.at[0, x], blk_1=p)

    def x_v(i):
        p = lax.rem(x + i, NX)
        lane = pl.ds(pl.multiple_of(p * HEAD_DIM, HEAD_DIM), HEAD_DIM)
        return remote(cv.at[:, lane], VA.at[own_rows, pl.ds(0, HEAD_DIM)], cs.at[1, p], cr.at[1, x], blk_1=p)

    l_q.wait()
    l_kv.wait()

    def y_wait(i):
        p = lax.rem(g + i, G)
        remote(q_in.at[p], qy.at[p], ys.at[0, p], yr.at[0, p], grp=p).wait_recv()
        remote(kv_in.at[p], kvy.at[p], ys.at[1, p], yr.at[1, p], grp=p).wait_recv()

    each(NX, lambda i: x_k(i).start())
    each(NX, lambda i: x_v(i).start())
    each(G, y_wait)

    def rows_of(sub):
        return pl.ds(pl.multiple_of(sub * G, G), G)

    def q_sub(zz, sub):
        return Q.at[zz, rows_of(sub)]

    def x_q(i):
        p = lax.rem(x + i, NX)
        return remote(qy.at[:, p], q_sub(z, x), xs.at[0, p], xr.at[0, x], blk_1=p)

    def x_kv(i):
        p = lax.rem(x + i, NX)
        return remote(kvy.at[:, p], kvn.at[rows_of(x)], xs.at[1, p], xr.at[1, x], blk_1=p)

    each(NX, lambda i: x_q(i).start())
    each(NX, lambda i: x_kv(i).start())

    def ag(way, step, sub, src=None):
        to = lax.rem(z + (1 if way == 0 else NZ - 1), NZ)
        held = lax.rem(z + ((NZ - step + 1) if way == 0 else (step - 1)), NZ)
        if src is None:
            src = q_sub(held, sub)
        return remote(src, q_sub(held, sub), ags.at[way, step - 1, sub], agr.at[way, step - 1, sub], blk_0=to)

    def ag_in(way, step, sub):
        to = lax.rem(z + (1 if way == 0 else NZ - 1), NZ)
        held = lax.rem(z + ((NZ - step) if way == 0 else step), NZ)
        return remote(q_sub(held, sub), q_sub(held, sub), ags.at[way, step - 1, sub], agr.at[way, step - 1, sub], blk_0=to)

    for way in (0, 1):
        ag(way, 1, x, src=qy.at[:, x]).start()
    Q[z, rows_of(x)] = qy[:, x]
    kvn[rows_of(x)] = kvy[:, x]

    def first_ring(i):
        p = lax.rem(x + i, NX)
        remote(qy.at[:, p], q_sub(z, p), xs.at[0, p], xr.at[0, p], blk_1=p).wait_recv()
        for way in (0, 1):
            ag(way, 1, p).start()

    each(NX, first_ring)

    def kv_wait(i):
        p = lax.rem(x + i, NX)
        remote(kvy.at[:, p], kvn.at[rows_of(p)], xs.at[1, p], xr.at[1, p], blk_1=p).wait_recv()

    each(NX, kv_wait)
    KN[0:T] = kvn[:, 0, :]
    VN[0:T, 0:HEAD_DIM] = kvn[:, 1, :]

    def cache_wait(i):
        p = lax.rem(x + i, NX)
        rows = pl.ds(pl.multiple_of(p * C, C), C)
        remote(ck.at[:, own_lane], K.at[rows], cs.at[0, p], cr.at[0, p], blk_1=p).wait_recv()
        remote(cv.at[:, own_lane], VA.at[rows, pl.ds(0, HEAD_DIM)], cs.at[1, p], cr.at[1, p], blk_1=p).wait_recv()

    l_k.wait()
    l_v.wait()
    each(NX, cache_wait)

    R = T * GROUP
    eye = lax.broadcasted_iota(jnp.int32, (GR, GR), 0) == lax.broadcasted_iota(jnp.int32, (GR, GR), 1)

    def position(token, block):
        pos = jnp.full(token.shape, 1 << 20, jnp.int32)
        for s in range(NX):
            here = (token >= s * G) & (token < (s + 1) * G)
            pos = jnp.where(here, assign[block * NX + s] * G + (token - s * G), pos)
        return pos

    def send_out(c):
        return (
            remote(OP.at[c], OR.at[z], os_.at[0, c], or_.at[0, z], blk_0=c),
            remote(LP.at[c], LR.at[z], os_.at[1, c], or_.at[1, z], blk_0=c),
        )

    def chunk(j, carry):
        step = (j + 1) // 2

        @pl.when(lax.rem(j, 2) == 1)
        def _():
            for sub in range(NX):
                for way in (0, 1):
                    mine = (sub < NX // 2) if way == 0 else (sub >= NX // 2)

                    def arrive(way=way, sub=sub):
                        ag_in(way, step, sub).wait_recv()

                    def onward(way=way, sub=sub):
                        ag(way, step + 1, sub).start()

                    if mine:
                        arrive()
                        pl.when(step < H)(onward)
                    else:
                        pl.when(step < H)(arrive)
                        pl.when(step < H - 1)(onward)

        c = lax.rem(jnp.where(lax.rem(j, 2) == 1, z + NZ - step, z + step), NZ)
        q = Q[c].reshape(R, HEAD_DIM)
        dn = (((1,), (1,)), ((), ()))
        s1 = lax.dot_general(q, K[...], dn, preferred_element_type=jnp.float32) + bias[...]
        s2 = lax.dot_general(q, KN[...], dn, preferred_element_type=jnp.float32)
        pt = position(lax.broadcasted_iota(jnp.int32, (R, 1), 0) // GROUP, c)
        pu = position(lax.broadcasted_iota(jnp.int32, (1, PN), 1), z)
        s2 = jnp.where(pu <= pt, s2, NEG)
        top = jnp.maximum(jnp.max(s1, axis=1, keepdims=True), jnp.max(s2, axis=1, keepdims=True))
        p1 = jnp.exp2((s1 - top) * TO_LOG2).astype(jnp.bfloat16)
        p2 = jnp.exp2((s2 - top) * TO_LOG2).astype(jnp.bfloat16)
        both = jnp.dot(p1, VA[...], preferred_element_type=jnp.float32)
        both = both + jnp.dot(p2, VN[...], preferred_element_type=jnp.float32)
        weight = both[:, HEAD_DIM:]
        OP[c] = (both[:, :HEAD_DIM] / weight).astype(jnp.bfloat16).reshape(T, GROUP, HEAD_DIM)
        level = (top * TO_LOG2 + jnp.log2(weight))[:, :GR]
        LP[c] = jnp.sum(jnp.where(eye[None], level.reshape(NX, GR, GR), 0.0), axis=1)

        @pl.when(j == 0)
        def _():
            OR[z] = OP[z]
            LR[z] = LP[z]

        @pl.when(j > 0)
        def _():
            for copy in send_out(c):
                copy.start()

        return carry

    lax.fori_loop(0, NZ, chunk, 0)

    def part_wait(i):
        b = lax.rem(z + i, NZ)
        remote(OP.at[b], OR.at[b], os_.at[0, b], or_.at[0, b], blk_0=b).wait_recv()
        remote(LP.at[b], LR.at[b], os_.at[1, b], or_.at[1, b], blk_0=b).wait_recv()

    each(NZ, part_wait)
    levels = LR[...]
    share = jnp.exp2(levels - jnp.max(levels, axis=0, keepdims=True))
    share = share / jnp.sum(share, axis=0, keepdims=True)
    slot = lax.broadcasted_iota(jnp.int32, (NX, GR), 0) * G + lax.broadcasted_iota(jnp.int32, (NX, GR), 1) // GROUP
    W[...] = jnp.where((position(slot, z) < counts[0])[None], share, 0.0)

    def x_out(p):
        return remote(res.at[rows_of(p)], OX.at[:, x], fs.at[p], fr.at[x], blk_1=p)

    def merge(i, carry):
        p = lax.rem(x + i, NX)
        total = jnp.zeros((GR, HEAD_DIM), jnp.float32)
        for b in range(NZ):
            w = jnp.sum(jnp.where(eye, W[b, pl.ds(p, 1), :], 0.0), axis=1, keepdims=True)
            total = total + w * OR[b, rows_of(p)].reshape(GR, HEAD_DIM).astype(jnp.float32)
        res[rows_of(p)] = total.astype(jnp.bfloat16).reshape(G, GROUP, HEAD_DIM)

        @pl.when(i < NX)
        def _():
            x_out(p).start()

        return carry

    lax.fori_loop(1, NX + 1, merge, 0)
    OX[:, x] = res[rows_of(x)]

    def x_out_wait(i):
        p = lax.rem(x + i, NX)
        remote(res.at[rows_of(p)], OX.at[:, p], fs.at[p], fr.at[p], blk_1=p).wait_recv()

    each(NX, x_out_wait)

    def y_out(i):
        p = lax.rem(g + i, G)
        return remote(OX.at[p], out.at[g], ts.at[p], tr.at[g], grp=p)

    each(G, lambda i: y_out(i).start())
    l_o = pltpu.make_async_copy(OX.at[g], out.at[g], loc.at[0])
    l_o.start()

    def y_out_wait(i):
        p = lax.rem(g + i, G)
        remote(OX.at[p], out.at[p], ts.at[p], tr.at[p], grp=p).wait_recv()

    each(G, y_out_wait)
    l_o.wait()

    each(G, lambda i: y_q(i).wait_send())
    each(G, lambda i: y_kv(i).wait_send())
    each(G, lambda i: y_out(i).wait_send())
    each(NX, lambda i: x_k(i).wait_send())
    each(NX, lambda i: x_v(i).wait_send())
    each(NX, lambda i: x_q(i).wait_send())
    each(NX, lambda i: x_kv(i).wait_send())
    each(NX, lambda i: x_out(lax.rem(x + i, NX)).wait_send())

    def part_sent(i):
        for copy in send_out(lax.rem(z + i, NZ)):
            copy.wait_send()

    each(NZ, part_sent)
    for way in (0, 1):
        for step in range(1, H + 1):
            for sub in range(NX):
                if step < H or ((sub < NX // 2) == (way == 0)):
                    ag(way, step, sub).wait_send()


def local(queries, cache_keys, cache_values, new_keys, new_values, hits, counts, assign):
    NZ, NX, G = lax.axis_size("blk_0"), lax.axis_size("blk_1"), lax.axis_size("grp")
    C = cache_keys.shape[1]
    T = NX * G
    PN = max(T, 128)
    N = NX * C
    q_in = queries.reshape(G, NX * GROUP, HEAD_DIM).reshape(G, NX, GROUP, HEAD_DIM)
    kv_in = jnp.stack(
        [new_keys.reshape(G, NX, HEAD_DIM), new_values.reshape(G, NX, HEAD_DIM)], axis=2
    )
    anywhere = pl.BlockSpec(memory_space=pl.ANY)
    smem = pl.BlockSpec(memory_space=pltpu.SMEM)
    bf, f32 = jnp.bfloat16, jnp.float32
    dma = pltpu.SemaphoreType.DMA
    made = pl.pallas_call(
        functools.partial(kernel, G, NZ, NX, C),
        out_shape=jax.ShapeDtypeStruct((G, NX, GROUP, HEAD_DIM), bf),
        in_specs=[anywhere] * 4 + [smem] * 3,
        out_specs=anywhere,
        scratch_shapes=[
            pltpu.VMEM((G, NX, GROUP, HEAD_DIM), bf),
            pltpu.VMEM((G, NX, 2, HEAD_DIM), bf),
            pltpu.VMEM((NZ, T, GROUP, HEAD_DIM), bf),
            pltpu.VMEM((N, HEAD_DIM), bf),
            pltpu.VMEM((N, 2 * HEAD_DIM), bf),
            pltpu.VMEM((T, 2, HEAD_DIM), bf),
            pltpu.VMEM((PN, HEAD_DIM), bf),
            pltpu.VMEM((PN, 2 * HEAD_DIM), bf),
            pltpu.VMEM((1, N), f32),
            pltpu.VMEM((NZ, T, GROUP, HEAD_DIM), bf),
            pltpu.VMEM((NZ, NX, G * GROUP), f32),
            pltpu.VMEM((NZ, T, GROUP, HEAD_DIM), bf),
            pltpu.VMEM((NZ, NX, G * GROUP), f32),
            pltpu.VMEM((NZ, NX, G * GROUP), f32),
            pltpu.VMEM((T, GROUP, HEAD_DIM), bf),
            pltpu.VMEM((G, NX, GROUP, HEAD_DIM), bf),
            dma((4,)),
            dma((2, G)), dma((2, G)),
            dma((2, NX)), dma((2, NX)),
            dma((2, NX)), dma((2, NX)),
            dma((2, NZ // 2, NX)), dma((2, NZ // 2, NX)),
            dma((2, NZ)), dma((2, NZ)),
            dma((NX,)), dma((NX,)),
            dma((G,)), dma((G,)),
        ],
        compiler_params=pltpu.CompilerParams(
            collective_id=0, has_side_effects=True, vmem_limit_bytes=56 * 1024 * 1024
        ),
        name="attend",
    )(q_in, kv_in, cache_keys[0], cache_values[0], hits, counts, assign[0])
    return made.reshape(G, 1, NX * GROUP * HEAD_DIM)


def solution(mesh):
    finer = Mesh(mesh.devices.reshape(mesh.shape["grp"], 8, 4), ("grp", "blk_0", "blk_1"))
    in_specs = (
        P(None, BLK_GRP, None),
        P("grp", BLK, None),
        P("grp", BLK, None),
        P(None, BLK_GRP, None),
        P(None, BLK_GRP, None),
        P("grp"),
        P("grp"),
        P("grp", None),
    )
    out_specs = P(None, BLK_GRP, None)
    return jax.shard_map(local, mesh=finer, in_specs=in_specs, out_specs=out_specs, check_vma=False)
```

```python
import functools

import jax
import jax.numpy as jnp
from jax import lax
from jax.experimental import pallas as pl
from jax.experimental.pallas import tpu as pltpu
from jax.sharding import Mesh
from jax.sharding import PartitionSpec as P

HEAD_DIM = 128
GROUP = 8
ONES = 16
BLK = ("blk_0", "blk_1")
BLK_GRP = ("blk_0", "blk_1", "grp")
NEG = -1e30
LOWEST = -3e38
TO_LOG2 = HEAD_DIM**-0.5 * 1.4426950408889634


def kernel(
    G, NZ, NX, C,
    q_hbm, nk_hbm, nv_hbm, ck, cv, hits_hbm, counts_hbm, assign_hbm,
    out,
    hits, counts, assign, q2, nk2, nv2, wide, q3, kvf, kv3, Q, KA, V, VT, kvn, S0, S1, M0, M1,
    SB, RB, SL, RL, res, out3, size,
    loc, sent_sem, q_sem, n_sem, cache_sem, ring_sem, part_sem, o_sem,
):
    g, z, x = lax.axis_index("grp"), lax.axis_index("blk_0"), lax.axis_index("blk_1")
    T = NX * G
    GR = G * GROUP
    HX = NX // 2
    HR = HX * GR
    N1 = NX * C
    NK = KA.shape[0]
    PN = NK - N1
    HEADS = NX * GROUP
    Y = G // 2
    H = NZ // 2
    f32, bf = jnp.float32, jnp.bfloat16

    def remote(src, dst, ssem, rsem, **where):
        return pltpu.make_async_remote_copy(
            src_ref=src, dst_ref=dst, send_sem=ssem, recv_sem=rsem,
            device_id=where, device_id_type=pl.DeviceIdType.MESH,
        )

    def loop(start, n, fn):
        def body(i, carry):
            fn(i)
            return carry
        lax.fori_loop(start, n, body, 0)

    def peer(i):
        k = i // 2
        far = jnp.where(k == 0, Y // 2, (Y - k) // 2)
        step = jnp.where(lax.rem(k, 2) == 1, far, Y - far)
        return lax.rem(g // 2 + step, Y) * 2 + lax.rem(g + 1 + i, 2)

    turns = [lax.rem(x + 1 + j, NX) for j in range(NX)]

    def others(fn):
        def one(i):
            p = peer(i)
            for t in turns:
                fn(p, t)
        loop(0, G - 1, one)
        for t in turns[:-1]:
            fn(g, t)

    barrier = pltpu.get_barrier_semaphore()

    def greet(**where):
        pl.semaphore_signal(barrier, 1, device_id=where, device_id_type=pl.DeviceIdType.MESH)

    others(lambda p, t: greet(grp=p, blk_1=t))
    after, before = lax.rem(z + 1, NZ), lax.rem(z + NZ - 1, NZ)
    greet(blk_0=after)
    greet(blk_0=before)
    greet(blk_0=lax.rem(z + H - 1, NZ))
    greet(blk_0=lax.rem(z + NZ - H + 1, NZ))

    own_lane = pl.ds(pl.multiple_of(x * HEAD_DIM, HEAD_DIM), HEAD_DIM)
    low = pl.ds(0, HEAD_DIM)

    def rows_from(p):
        return pl.ds(pl.multiple_of(p * C, C), C)

    ins = [
        pltpu.make_async_copy(q_hbm, q2, loc.at[0]),
        pltpu.make_async_copy(nk_hbm, nk2, loc.at[1]),
        pltpu.make_async_copy(nv_hbm, nv2, loc.at[2]),
        pltpu.make_async_copy(ck.at[:, own_lane], KA.at[rows_from(x), low], loc.at[3]),
        pltpu.make_async_copy(cv.at[:, own_lane], V.at[rows_from(x)], loc.at[4]),
        pltpu.make_async_copy(hits_hbm, hits, loc.at[5]),
        pltpu.make_async_copy(counts_hbm, counts, loc.at[6]),
        pltpu.make_async_copy(assign_hbm, assign, loc.at[7]),
    ]
    for c in ins:
        c.start()

    ins[0].wait()
    for h in range(HEADS):
        wide[pl.ds(h, G, stride=HEADS), :] = q2[:, h * HEAD_DIM : (h + 1) * HEAD_DIM].astype(f32)
    q3[...] = wide[...].astype(bf).reshape(G, NX, GROUP, HEAD_DIM)
    ins[1].wait()
    ins[2].wait()
    for h in range(NX):
        cut = slice(h * HEAD_DIM, (h + 1) * HEAD_DIM)
        kvf[pl.ds(2 * h, G, stride=2 * NX), :] = nk2[:, cut].astype(f32)
        kvf[pl.ds(2 * h + 1, G, stride=2 * NX), :] = nv2[:, cut].astype(f32)
    kv3[...] = kvf[...].reshape(G, NX, 2, HEAD_DIM).astype(bf)

    pl.semaphore_wait(barrier, G * NX - 1 + 4)

    def q_copy(p, t):
        return remote(q3.at[p, t], Q.at[z, x * G + g], sent_sem.at[0], q_sem.at[x], grp=p, blk_1=t)

    def n_copy(p, t):
        return remote(kv3.at[p, t], kvn.at[x * G + g], sent_sem.at[1], n_sem.at[0], grp=p, blk_1=t)

    def landed(ref, sem):
        pltpu.make_async_copy(ref, ref, sem).wait()

    def k_copy(i):
        p = lax.rem(x + i, NX)
        lane = pl.ds(pl.multiple_of(p * HEAD_DIM, HEAD_DIM), HEAD_DIM)
        return remote(ck.at[:, lane], KA.at[rows_from(x), low], sent_sem.at[2], cache_sem.at[0], blk_1=p)

    def v_copy(i):
        p = lax.rem(x + i, NX)
        lane = pl.ds(pl.multiple_of(p * HEAD_DIM, HEAD_DIM), HEAD_DIM)
        return remote(cv.at[:, lane], V.at[rows_from(x)], sent_sem.at[2], cache_sem.at[1], blk_1=p)

    others(lambda p, t: q_copy(p, t).start())
    others(lambda p, t: n_copy(p, t).start())
    loop(1, NX, lambda i: k_copy(i).start())
    loop(1, NX, lambda i: v_copy(i).start())

    Q[z, x * G + g] = q3[g, x]
    kvn[x * G + g] = kv3[g, x]

    for c in ins[5:]:
        c.wait()
    limit = hits[0] - z * N1
    row = lax.broadcasted_iota(jnp.int32, (NK, HEAD_DIM), 0)
    lane0 = lax.broadcasted_iota(jnp.int32, (NK, HEAD_DIM), 1) == 0
    barred = lane0 & (row >= limit) & (row < N1)
    KA[:, HEAD_DIM:] = jnp.where(barred, NEG, 0.0).astype(bf)
    KA[N1:, 0:HEAD_DIM] = jnp.zeros((PN, HEAD_DIM), bf)
    V[N1:, :] = jnp.zeros((PN, HEAD_DIM), bf)
    VT[HEAD_DIM:, :] = jnp.ones((ONES, NK), bf)
    for way in (0, 1):
        for s in range(HX):
            for k in (0, H):
                RB[way, k, s] = jnp.zeros((HEAD_DIM, GR), bf)
                RL[way, k, s] = jnp.full((1, GR), LOWEST, f32)

    def held(way, k):
        return lax.rem(z + (NZ - k if way == 0 else k), NZ)

    def go(way):
        return after if way == 0 else before

    def q_rows(way, k, s):
        return Q.at[held(way, k), pl.ds((way * HX + s) * G, G)]

    def q_on(way, k, s):
        ref = q_rows(way, k, s)
        return remote(ref, ref, sent_sem.at[3], ring_sem.at[way, k, s], blk_0=go(way))

    for s in range(HX):
        for way in (0, 1):
            t = way * HX + s

            @pl.when(x == t)
            def _():
                landed(Q.at[z, pl.ds(t * G, G - 1)], q_sem.at[t])

            @pl.when(x != t)
            def _():
                landed(Q.at[z, pl.ds(t * G, G)], q_sem.at[t])

            q_on(way, 0, s).start()

    def pass_on(k):
        for s in range(HX):
            for way in (0, 1):
                landed(q_rows(way, k, s), ring_sem.at[way, k - 1, s])
                if isinstance(k, int):
                    q_on(way, k, s).start()
                else:
                    pl.when(k < NZ - 1)(lambda way=way, s=s: q_on(way, k, s).start())

    for k in range(1, H):
        pass_on(k)

    landed(kvn.at[pl.ds(0, T - 1)], n_sem.at[0])
    KA[N1 : N1 + T, 0:HEAD_DIM] = kvn[:, 0, :]
    V[N1 : N1 + T, :] = kvn[:, 1, :]
    ins[3].wait()
    landed(V.at[pl.ds(0, (NX - 1) * C)], cache_sem.at[0])

    def position(token, block):
        pos = jnp.full(token.shape, 1 << 20, jnp.int32)
        for s in range(NX):
            here = (token >= s * G) & (token < (s + 1) * G)
            pos = jnp.where(here, assign[block * NX + s] * G + (token - s * G), pos)
        return pos

    first = (lax.broadcasted_iota(jnp.int32, (HR, HEAD_DIM), 1) == 0).astype(f32).astype(bf)

    def scores(k, way, S, M):
        c = held(way, k)
        q = Q[c, pl.ds(way * HX * G, HX * G)].reshape(HR, HEAD_DIM)
        q = jnp.concatenate([q, first], axis=1)
        s = lax.dot_general(KA[...], q, (((1,), (1,)), ((), ())), preferred_element_type=f32)
        pt = position(way * HX * G + lax.broadcasted_iota(jnp.int32, (1, HR), 1) // GROUP, c)
        pu = position(lax.broadcasted_iota(jnp.int32, (PN, 1), 0), z)
        old, new = s[:N1], jnp.where(pu <= pt, s[N1:], NEG)
        S[0:N1] = old
        S[N1:] = new
        M[...] = jnp.maximum(
            jnp.max(old.reshape(N1 // 8, 8, HR), axis=0), jnp.max(new.reshape(PN // 8, 8, HR), axis=0)
        )

    def part_on(way, k, s):
        back = k == H - 1
        slot = jnp.where(back, NZ + 1, k + 1)
        to = jnp.where(back, held(way, k), go(way))
        return (
            remote(SB.at[way, k, s], RB.at[way, slot, s], sent_sem.at[4], part_sem.at[way, k, s], blk_0=to),
            remote(SL.at[way, k, s], RL.at[way, slot, s], sent_sem.at[5], part_sem.at[way, k, s], blk_0=to),
        )

    def part_in(way, k, s):
        landed(size, part_sem.at[way, k - 1, s])

    def blend(k, way, S, M):
        top = jnp.max(M[...], axis=0, keepdims=True)
        p = jnp.exp2((S[...] - top) * TO_LOG2).astype(bf)
        both = jnp.dot(VT[...], p, preferred_element_type=f32)
        weight = both[HEAD_DIM : HEAD_DIM + 1]
        level = top * TO_LOG2 + jnp.log2(weight)
        inverse = 1.0 / weight
        for s in range(HX):
            cut = slice(s * GR, (s + 1) * GR)

            @pl.when((k > 0) & (k != H))
            def _():
                part_in(way, k, s)

            there, here = RL[way, k, s], level[:, cut]
            high = jnp.maximum(there, here)
            a, b = jnp.exp2(there - high), jnp.exp2(here - high)
            both_parts = a + b
            a, b = a / both_parts, b / both_parts * inverse[:, cut]
            merged = RB[way, k, s].astype(f32) * a + both[:HEAD_DIM, cut] * b
            SB[way, k, s] = merged.astype(bf)
            SL[way, k, s] = high + jnp.log2(both_parts)
            for copy in part_on(way, k, s):
                copy.start()

    scores(0, 0, S0, M0)
    ins[4].wait()
    landed(V.at[pl.ds(0, (NX - 1) * C)], cache_sem.at[1])
    VT[0:HEAD_DIM, :] = V[...].T

    def turn(n):
        k = n // 2 + lax.rem(n, 2) * H
        m = jnp.minimum(n + 1, NZ - 1)
        m = m // 2 + lax.rem(m, 2) * H
        scores(k, 1, S1, M1)
        blend(k, 0, S0, M0)

        @pl.when((m >= H) & (n < NZ - 1))
        def _():
            pass_on(m)

        scores(m, 0, S0, M0)
        blend(k, 1, S1, M1)

    loop(0, NZ, turn)

    def o_copy(p, t):
        return remote(res.at[t * G + p], out3.at[g, x], sent_sem.at[6], o_sem.at[0], grp=p, blk_1=t)

    for s in range(HX):
        for way in (0, 1):
            t = way * HX + s
            part_in(way, H, s)
            part_in(way, NZ, s)
            one, two = RL[way, NZ, s], RL[way, NZ + 1, s]
            high = jnp.maximum(one, two)
            a, b = jnp.exp2(one - high), jnp.exp2(two - high)
            done = (RB[way, NZ, s].astype(f32) * a + RB[way, NZ + 1, s].astype(f32) * b) / (a + b)
            done = done.T
            place = assign[z * NX + t] * G + lax.broadcasted_iota(jnp.int32, (GR, 1), 0) // GROUP
            done = jnp.where(place < counts[0], done, 0.0).astype(bf)
            res[t * G : (t + 1) * G] = done.reshape(G, GROUP, HEAD_DIM)

            def give(i, t=t):
                p = peer(i)

                @pl.when((p != g) | (x != t))
                def _():
                    o_copy(p, t).start()

            loop(0, G, give)
    out3[g, x] = res[x * G + g]
    landed(res.at[pl.ds(0, T - 1)], o_sem.at[0])
    wide[...] = out3[...].reshape(G * HEADS, HEAD_DIM).astype(f32)
    for h in range(HEADS):
        out[:, h * HEAD_DIM : (h + 1) * HEAD_DIM] = wide[pl.ds(h, G, stride=HEADS), :].astype(bf)

    landed(res.at[pl.ds(0, T - 1)], sent_sem.at[0])
    landed(kvn.at[pl.ds(0, T - 1)], sent_sem.at[1])
    landed(KA.at[pl.ds(0, (NX - 1) * C)], sent_sem.at[2])
    landed(Q.at[pl.ds(0, NZ - 1), pl.ds(0, 2 * HX * G)], sent_sem.at[3])
    landed(SB, sent_sem.at[4])
    landed(SL, sent_sem.at[5])
    landed(res.at[pl.ds(0, T - 1)], sent_sem.at[6])


def local(queries, cache_keys, cache_values, new_keys, new_values, hits, counts, assign):
    NZ, NX, G = lax.axis_size("blk_0"), lax.axis_size("blk_1"), lax.axis_size("grp")
    C = cache_keys.shape[1]
    T = NX * G
    GR = G * GROUP
    HX = NX // 2
    HR = HX * GR
    N1 = NX * C
    NK = N1 + max(T, 128)
    W = NX * GROUP * HEAD_DIM
    hbm = pl.BlockSpec(memory_space=pltpu.HBM)
    bf, f32 = jnp.bfloat16, jnp.float32
    dma = pltpu.SemaphoreType.DMA
    held = (
        queries.reshape(G, W), new_keys.reshape(G, NX * HEAD_DIM), new_values.reshape(G, NX * HEAD_DIM),
        cache_keys[0], cache_values[0],
    )
    made = pl.pallas_call(
        functools.partial(kernel, G, NZ, NX, C),
        out_shape=jax.ShapeDtypeStruct((G, W), bf),
        in_specs=[hbm] * 8,
        out_specs=pl.BlockSpec(memory_space=pltpu.VMEM),
        scratch_shapes=[
            pltpu.SMEM((1,), jnp.int32),
            pltpu.SMEM((1,), jnp.int32),
            pltpu.SMEM((NZ * NX,), jnp.int32),
            pltpu.VMEM((G, W), bf),
            pltpu.VMEM((G, NX * HEAD_DIM), bf),
            pltpu.VMEM((G, NX * HEAD_DIM), bf),
            pltpu.VMEM((G * NX * GROUP, HEAD_DIM), f32),
            pltpu.VMEM((G, NX, GROUP, HEAD_DIM), bf),
            pltpu.VMEM((G * NX * 2, HEAD_DIM), f32),
            pltpu.VMEM((G, NX, 2, HEAD_DIM), bf),
            pltpu.VMEM((NZ, T, GROUP, HEAD_DIM), bf),
            pltpu.VMEM((NK, 2 * HEAD_DIM), bf),
            pltpu.VMEM((NK, HEAD_DIM), bf),
            pltpu.VMEM((HEAD_DIM + ONES, NK), bf),
            pltpu.VMEM((T, 2, HEAD_DIM), bf),
            pltpu.VMEM((NK, HR), f32),
            pltpu.VMEM((NK, HR), f32),
            pltpu.VMEM((8, HR), f32),
            pltpu.VMEM((8, HR), f32),
            pltpu.VMEM((2, NZ, HX, HEAD_DIM, GR), bf),
            pltpu.VMEM((2, NZ + 2, HX, HEAD_DIM, GR), bf),
            pltpu.VMEM((2, NZ, HX, 1, GR), f32),
            pltpu.VMEM((2, NZ + 2, HX, 1, GR), f32),
            pltpu.VMEM((T, GROUP, HEAD_DIM), bf),
            pltpu.VMEM((G, NX, GROUP, HEAD_DIM), bf),
            pltpu.VMEM((HEAD_DIM // 2 + 1, 1, GR), f32),
            dma((8,)), dma((7,)), dma((NX,)), dma((1,)), dma((2,)),
            dma((2, NZ - 1, HX)), dma((2, NZ, HX)), dma((1,)),
        ],
        compiler_params=pltpu.CompilerParams(
            collective_id=0, has_side_effects=True, vmem_limit_bytes=48 * 1024 * 1024
        ),
        name="attend",
    )(
        *(pltpu.with_memory_space_constraint(a, pltpu.HBM) for a in held), hits, counts,
        pltpu.with_memory_space_constraint(assign[0], pltpu.HBM),
    )
    return made.reshape(G, 1, W)


def solution(mesh):
    finer = Mesh(mesh.devices.reshape(mesh.shape["grp"], 8, 4), ("grp", "blk_0", "blk_1"))
    in_specs = (
        P(None, BLK_GRP, None),
        P("grp", BLK, None),
        P("grp", BLK, None),
        P(None, BLK_GRP, None),
        P(None, BLK_GRP, None),
        P("grp"),
        P("grp"),
        P("grp", None),
    )
    out_specs = P(None, BLK_GRP, None)
    return jax.shard_map(local, mesh=finer, in_specs=in_specs, out_specs=out_specs, check_vma=False)
```

```python
import functools

import jax
import jax.numpy as jnp
from jax import lax
from jax.experimental import pallas as pl
from jax.experimental.pallas import tpu as pltpu
from jax.sharding import Mesh
from jax.sharding import PartitionSpec as P

HEAD_DIM = 128
GROUP = 8
ONES = 16
BLK = ("blk_0", "blk_1")
BLK_GRP = ("blk_0", "blk_1", "grp")
NEG = -1e30
LOWEST = -3e38
TO_LOG2 = HEAD_DIM**-0.5 * 1.4426950408889634


def kernel(
    G, NZ, NX, C,
    q_hbm, nk_hbm, nv_hbm, ck, cv, hits_hbm, counts_hbm, assign_hbm,
    out,
    hits, counts, assign, q2, nk2, nv2, wide, q3, kvf, kv3, Q, KA, V, VT, kvn, S0, S1, M0, M1,
    SB, RB, SL, RL, res, out3, size,
    loc, sent_sem, q_sem, n_sem, cache_sem, ring_sem, part_sem, o_sem,
):
    g, z, x = lax.axis_index("grp"), lax.axis_index("blk_0"), lax.axis_index("blk_1")
    T = NX * G
    GR = G * GROUP
    HX = NX // 2
    HR = HX * GR
    N1 = NX * C
    NK = KA.shape[0]
    PN = NK - N1
    HEADS = NX * GROUP
    Y = G // 2
    H = NZ // 2
    f32, bf = jnp.float32, jnp.bfloat16

    def remote(src, dst, ssem, rsem, **where):
        return pltpu.make_async_remote_copy(
            src_ref=src, dst_ref=dst, send_sem=ssem, recv_sem=rsem,
            device_id=where, device_id_type=pl.DeviceIdType.MESH,
        )

    def loop(start, n, fn):
        def body(i, carry):
            fn(i)
            return carry
        lax.fori_loop(start, n, body, 0)

    def peer(i):
        k = i // 2
        far = jnp.where(k == 0, Y // 2, (Y - k) // 2)
        step = jnp.where(lax.rem(k, 2) == 1, far, Y - far)
        return lax.rem(g // 2 + step, Y) * 2 + lax.rem(g + 1 + i, 2)

    turns = [lax.rem(x + 1 + j, NX) for j in range(NX)]

    def others(fn):
        def one(i):
            p = peer(i)
            for t in turns:
                fn(p, t)
        loop(0, G - 1, one)
        for t in turns[:-1]:
            fn(g, t)

    barrier = pltpu.get_barrier_semaphore()

    def greet(**where):
        pl.semaphore_signal(barrier, 1, device_id=where, device_id_type=pl.DeviceIdType.MESH)

    others(lambda p, t: greet(grp=p, blk_1=t))
    after, before = lax.rem(z + 1, NZ), lax.rem(z + NZ - 1, NZ)
    greet(blk_0=after)
    greet(blk_0=before)
    greet(blk_0=lax.rem(z + 2, NZ))
    greet(blk_0=lax.rem(z + NZ - 2, NZ))

    own_lane = pl.ds(pl.multiple_of(x * HEAD_DIM, HEAD_DIM), HEAD_DIM)
    low = pl.ds(0, HEAD_DIM)

    def rows_from(p):
        return pl.ds(pl.multiple_of(p * C, C), C)

    ins = [
        pltpu.make_async_copy(q_hbm, q2, loc.at[0]),
        pltpu.make_async_copy(nk_hbm, nk2, loc.at[1]),
        pltpu.make_async_copy(nv_hbm, nv2, loc.at[2]),
        pltpu.make_async_copy(ck.at[:, own_lane], KA.at[rows_from(x), low], loc.at[3]),
        pltpu.make_async_copy(cv.at[:, own_lane], V.at[rows_from(x)], loc.at[4]),
        pltpu.make_async_copy(hits_hbm, hits, loc.at[5]),
        pltpu.make_async_copy(counts_hbm, counts, loc.at[6]),
        pltpu.make_async_copy(assign_hbm, assign, loc.at[7]),
    ]
    for c in ins:
        c.start()

    ins[0].wait()
    for h in range(HEADS):
        wide[pl.ds(h, G, stride=HEADS), :] = q2[:, h * HEAD_DIM : (h + 1) * HEAD_DIM].astype(f32)
    q3[...] = wide[...].astype(bf).reshape(G, NX, GROUP, HEAD_DIM)
    ins[1].wait()
    ins[2].wait()
    for h in range(NX):
        cut = slice(h * HEAD_DIM, (h + 1) * HEAD_DIM)
        kvf[pl.ds(2 * h, G, stride=2 * NX), :] = nk2[:, cut].astype(f32)
        kvf[pl.ds(2 * h + 1, G, stride=2 * NX), :] = nv2[:, cut].astype(f32)
    kv3[...] = kvf[...].reshape(G, NX, 2, HEAD_DIM).astype(bf)

    pl.semaphore_wait(barrier, G * NX - 1 + 4)

    def q_copy(p, t):
        return remote(q3.at[p, t], Q.at[z, x * G + g], sent_sem.at[0], q_sem.at[x], grp=p, blk_1=t)

    def n_copy(p, t):
        return remote(kv3.at[p, t], kvn.at[x * G + g], sent_sem.at[1], n_sem.at[0], grp=p, blk_1=t)

    def landed(ref, sem):
        pltpu.make_async_copy(ref, ref, sem).wait()

    def k_copy(i):
        p = lax.rem(x + i, NX)
        lane = pl.ds(pl.multiple_of(p * HEAD_DIM, HEAD_DIM), HEAD_DIM)
        return remote(ck.at[:, lane], KA.at[rows_from(x), low], sent_sem.at[2], cache_sem.at[0], blk_1=p)

    def v_copy(i):
        p = lax.rem(x + i, NX)
        lane = pl.ds(pl.multiple_of(p * HEAD_DIM, HEAD_DIM), HEAD_DIM)
        return remote(cv.at[:, lane], V.at[rows_from(x)], sent_sem.at[2], cache_sem.at[1], blk_1=p)

    others(lambda p, t: q_copy(p, t).start())
    loop(1, NX, lambda i: k_copy(i).start())
    others(lambda p, t: n_copy(p, t).start())
    loop(1, NX, lambda i: v_copy(i).start())

    Q[z, x * G + g] = q3[g, x]
    kvn[x * G + g] = kv3[g, x]

    for c in ins[5:]:
        c.wait()
    limit = hits[0] - z * N1
    row = lax.broadcasted_iota(jnp.int32, (NK, HEAD_DIM), 0)
    lane0 = lax.broadcasted_iota(jnp.int32, (NK, HEAD_DIM), 1) == 0
    barred = lane0 & (row >= limit) & (row < N1)
    KA[:, HEAD_DIM:] = jnp.where(barred, NEG, 0.0).astype(bf)
    KA[N1:, 0:HEAD_DIM] = jnp.zeros((PN, HEAD_DIM), bf)
    V[N1:, :] = jnp.zeros((PN, HEAD_DIM), bf)
    VT[HEAD_DIM:, :] = jnp.ones((ONES, NK), bf)
    for way in (0, 1):
        for s in range(HX):
            RB[way, NZ + 1, s] = jnp.zeros((HEAD_DIM, GR), bf)
            RL[way, NZ + 1, s] = jnp.full((1, GR), LOWEST, f32)

    def held(way, k):
        return lax.rem(z + (NZ - k if way == 0 else k), NZ)

    def go(way):
        return after if way == 0 else before

    def q_rows(way, k, s):
        return Q.at[held(way, k), pl.ds((way * HX + s) * G, G)]

    routes = {0: (2, 1), 2: (4, 3), 4: (5,), 5: (6,), 6: (7,)} if NZ == 8 else {0: (2, 1), 2: (3,)}
    due = {4: (4,), 3: (3,), 5: (5,), 6: (6,), 1: (1,), 7: (7,)} if NZ == 8 else {2: (2,), 1: (1,), 3: (3,)}

    def q_on(way, k, s, hop):
        ref = q_rows(way, k, s)
        to = lax.rem(z + (hop if way == 0 else NZ - hop), NZ)
        return remote(ref, ref, sent_sem.at[3], ring_sem.at[way, k + hop - 1, s], blk_0=to)

    for s in range(HX):
        for way in (0, 1):
            t = way * HX + s

            @pl.when(x == t)
            def _():
                landed(Q.at[z, pl.ds(t * G, G - 1)], q_sem.at[t])

            @pl.when(x != t)
            def _():
                landed(Q.at[z, pl.ds(t * G, G)], q_sem.at[t])

            q_on(way, 0, s, 2).start()

    def pass_on(k):
        for s in range(HX):
            for way in (0, 1):
                landed(q_rows(way, k, s), ring_sem.at[way, k - 1, s])
                for further in routes.get(k, ())[:1]:
                    q_on(way, k, s, further - k).start()
        for further in routes.get(k, ())[1:]:
            for s in range(HX):
                for way in (0, 1):
                    q_on(way, k, s, further - k).start()

    for k in range(2, H, 2):
        pass_on(k)
    for s in range(HX):
        for way in (0, 1):
            q_on(way, 0, s, 1).start()

    landed(kvn.at[pl.ds(0, T - 1)], n_sem.at[0])
    KA[N1 : N1 + T, 0:HEAD_DIM] = kvn[:, 0, :]
    V[N1 : N1 + T, :] = kvn[:, 1, :]
    ins[3].wait()
    landed(V.at[pl.ds(0, (NX - 1) * C)], cache_sem.at[0])

    def position(token, block):
        pos = jnp.full(token.shape, 1 << 20, jnp.int32)
        for s in range(NX):
            here = (token >= s * G) & (token < (s + 1) * G)
            pos = jnp.where(here, assign[block * NX + s] * G + (token - s * G), pos)
        return pos

    first = (lax.broadcasted_iota(jnp.int32, (HR, HEAD_DIM), 1) == 0).astype(f32).astype(bf)

    def scores(k, way, S, M):
        c = held(way, k)
        q = Q[c, pl.ds(way * HX * G, HX * G)].reshape(HR, HEAD_DIM)
        q = jnp.concatenate([q, first], axis=1)
        s = lax.dot_general(KA[...], q, (((1,), (1,)), ((), ())), preferred_element_type=f32)
        pt = position(way * HX * G + lax.broadcasted_iota(jnp.int32, (1, HR), 1) // GROUP, c)
        pu = position(lax.broadcasted_iota(jnp.int32, (PN, 1), 0), z)
        old, new = s[:N1], jnp.where(pu <= pt, s[N1:], NEG)
        S[0:N1] = old
        S[N1:] = new
        M[...] = jnp.maximum(
            jnp.max(old.reshape(N1 // 8, 8, HR), axis=0), jnp.max(new.reshape(PN // 8, 8, HR), axis=0)
        )

    def part_on(way, k, s):
        slot = jnp.where(k >= H, k + 1, k - 1)
        to = jnp.where(k >= H, go(way), go(1 - way))
        return (
            remote(SB.at[way, k, s], RB.at[way, slot, s], sent_sem.at[4], part_sem.at[way, slot, s], blk_0=to),
            remote(SL.at[way, k, s], RL.at[way, slot, s], sent_sem.at[5], part_sem.at[way, slot, s], blk_0=to),
        )

    def part_in(way, slot, s):
        landed(size, part_sem.at[way, slot, s])

    def blend(k, way, S, M):
        top = jnp.max(M[...], axis=0, keepdims=True)
        p = jnp.exp2((S[...] - top) * TO_LOG2).astype(bf)
        both = jnp.dot(VT[...], p, preferred_element_type=f32)
        weight = both[HEAD_DIM : HEAD_DIM + 1]
        level = top * TO_LOG2 + jnp.log2(weight)
        inverse = 1.0 / weight
        fresh = (k == 0) | (k == H - 1) | (k == H)
        slot = jnp.where(fresh, NZ + 1, k)
        for s in range(HX):
            cut = slice(s * GR, (s + 1) * GR)

            @pl.when(jnp.logical_not(fresh))
            def _():
                part_in(way, k, s)

            there, here = RL[way, slot, s], level[:, cut]
            high = jnp.maximum(there, here)
            a, b = jnp.exp2(there - high), jnp.exp2(here - high)
            both_parts = a + b
            a, b = a / both_parts, b / both_parts * inverse[:, cut]
            merged = RB[way, slot, s].astype(f32) * a + both[:HEAD_DIM, cut] * b
            SB[way, k, s] = merged.astype(bf)
            SL[way, k, s] = high + jnp.log2(both_parts)

            @pl.when(k > 0)
            def _():
                for copy in part_on(way, k, s):
                    copy.start()

    scores(0, 0, S0, M0)
    ins[4].wait()
    landed(V.at[pl.ds(0, (NX - 1) * C)], cache_sem.at[1])
    VT[0:HEAD_DIM, :] = V[...].T

    def step_of(n):
        return jnp.where(lax.rem(n, 2) == 1, H + n // 2, jnp.where(n == 0, 0, H - n // 2))

    def turn(n):
        k, m = step_of(n), step_of(jnp.minimum(n + 1, NZ - 1))
        scores(k, 1, S1, M1)
        blend(k, 0, S0, M0)
        for at, steps in due.items():

            @pl.when((m == at) & (n < NZ - 1))
            def _():
                for step in steps:
                    pass_on(step)

        scores(m, 0, S0, M0)
        blend(k, 1, S1, M1)

    loop(0, NZ, turn)

    def o_copy(p, t):
        return remote(res.at[t * G + p], out3.at[g, x], sent_sem.at[6], o_sem.at[0], grp=p, blk_1=t)

    for s in range(HX):
        for way in (0, 1):
            t = way * HX + s
            part_in(way, 0, s)
            part_in(way, NZ, s)
            one, two, own = RL[way, 0, s], RL[way, NZ, s], SL[way, 0, s]
            high = jnp.maximum(jnp.maximum(one, two), own)
            a, b, c = jnp.exp2(one - high), jnp.exp2(two - high), jnp.exp2(own - high)
            done = RB[way, 0, s].astype(f32) * a + RB[way, NZ, s].astype(f32) * b
            done = (done + SB[way, 0, s].astype(f32) * c) / (a + b + c)
            done = done.T
            place = assign[z * NX + t] * G + lax.broadcasted_iota(jnp.int32, (GR, 1), 0) // GROUP
            done = jnp.where(place < counts[0], done, 0.0).astype(bf)
            res[t * G : (t + 1) * G] = done.reshape(G, GROUP, HEAD_DIM)

            def give(i, t=t):
                p = peer(i)

                @pl.when((p != g) | (x != t))
                def _():
                    o_copy(p, t).start()

            loop(0, G, give)
    out3[g, x] = res[x * G + g]
    landed(res.at[pl.ds(0, T - 1)], o_sem.at[0])
    wide[...] = out3[...].reshape(G * HEADS, HEAD_DIM).astype(f32)
    for h in range(HEADS):
        out[:, h * HEAD_DIM : (h + 1) * HEAD_DIM] = wide[pl.ds(h, G, stride=HEADS), :].astype(bf)

    landed(res.at[pl.ds(0, T - 1)], sent_sem.at[0])
    landed(kvn.at[pl.ds(0, T - 1)], sent_sem.at[1])
    landed(KA.at[pl.ds(0, (NX - 1) * C)], sent_sem.at[2])
    landed(Q.at[pl.ds(0, NZ - 1), pl.ds(0, 2 * HX * G)], sent_sem.at[3])
    landed(SB.at[:, pl.ds(1, NZ - 1)], sent_sem.at[4])
    landed(SL.at[:, pl.ds(1, NZ - 1)], sent_sem.at[5])
    landed(res.at[pl.ds(0, T - 1)], sent_sem.at[6])


def local(queries, cache_keys, cache_values, new_keys, new_values, hits, counts, assign):
    NZ, NX, G = lax.axis_size("blk_0"), lax.axis_size("blk_1"), lax.axis_size("grp")
    C = cache_keys.shape[1]
    T = NX * G
    GR = G * GROUP
    HX = NX // 2
    HR = HX * GR
    N1 = NX * C
    NK = N1 + max(T, 128)
    W = NX * GROUP * HEAD_DIM
    hbm = pl.BlockSpec(memory_space=pltpu.HBM)
    bf, f32 = jnp.bfloat16, jnp.float32
    dma = pltpu.SemaphoreType.DMA
    held = (
        queries.reshape(G, W), new_keys.reshape(G, NX * HEAD_DIM), new_values.reshape(G, NX * HEAD_DIM),
        cache_keys[0], cache_values[0],
    )
    made = pl.pallas_call(
        functools.partial(kernel, G, NZ, NX, C),
        out_shape=jax.ShapeDtypeStruct((G, W), bf),
        in_specs=[hbm] * 8,
        out_specs=pl.BlockSpec(memory_space=pltpu.VMEM),
        scratch_shapes=[
            pltpu.SMEM((1,), jnp.int32),
            pltpu.SMEM((1,), jnp.int32),
            pltpu.SMEM((NZ * NX,), jnp.int32),
            pltpu.VMEM((G, W), bf),
            pltpu.VMEM((G, NX * HEAD_DIM), bf),
            pltpu.VMEM((G, NX * HEAD_DIM), bf),
            pltpu.VMEM((G * NX * GROUP, HEAD_DIM), f32),
            pltpu.VMEM((G, NX, GROUP, HEAD_DIM), bf),
            pltpu.VMEM((G * NX * 2, HEAD_DIM), f32),
            pltpu.VMEM((G, NX, 2, HEAD_DIM), bf),
            pltpu.VMEM((NZ, T, GROUP, HEAD_DIM), bf),
            pltpu.VMEM((NK, 2 * HEAD_DIM), bf),
            pltpu.VMEM((NK, HEAD_DIM), bf),
            pltpu.VMEM((HEAD_DIM + ONES, NK), bf),
            pltpu.VMEM((T, 2, HEAD_DIM), bf),
            pltpu.VMEM((NK, HR), f32),
            pltpu.VMEM((NK, HR), f32),
            pltpu.VMEM((8, HR), f32),
            pltpu.VMEM((8, HR), f32),
            pltpu.VMEM((2, NZ, HX, HEAD_DIM, GR), bf),
            pltpu.VMEM((2, NZ + 2, HX, HEAD_DIM, GR), bf),
            pltpu.VMEM((2, NZ, HX, 1, GR), f32),
            pltpu.VMEM((2, NZ + 2, HX, 1, GR), f32),
            pltpu.VMEM((T, GROUP, HEAD_DIM), bf),
            pltpu.VMEM((G, NX, GROUP, HEAD_DIM), bf),
            pltpu.VMEM((HEAD_DIM // 2 + 1, 1, GR), f32),
            dma((8,)), dma((7,)), dma((NX,)), dma((1,)), dma((2,)),
            dma((2, NZ - 1, HX)), dma((2, NZ + 1, HX)), dma((1,)),
        ],
        compiler_params=pltpu.CompilerParams(
            collective_id=0, has_side_effects=True, vmem_limit_bytes=48 * 1024 * 1024
        ),
        name="attend",
    )(
        *(pltpu.with_memory_space_constraint(a, pltpu.HBM) for a in held), hits, counts,
        pltpu.with_memory_space_constraint(assign[0], pltpu.HBM),
    )
    return made.reshape(G, 1, W)


def solution(mesh):
    finer = Mesh(mesh.devices.reshape(mesh.shape["grp"], 8, 4), ("grp", "blk_0", "blk_1"))
    in_specs = (
        P(None, BLK_GRP, None),
        P("grp", BLK, None),
        P("grp", BLK, None),
        P(None, BLK_GRP, None),
        P(None, BLK_GRP, None),
        P("grp"),
        P("grp"),
        P("grp", None),
    )
    out_specs = P(None, BLK_GRP, None)
    return jax.shard_map(local, mesh=finer, in_specs=in_specs, out_specs=out_specs, check_vma=False)
```

```python
import functools

import jax
import jax.numpy as jnp
from jax import lax
from jax.experimental import pallas as pl
from jax.experimental.pallas import tpu as pltpu
from jax.sharding import Mesh
from jax.sharding import PartitionSpec as P

HEAD_DIM = 128
GROUP = 8
ONES = 16
BLK = ("blk_0", "blk_1")
BLK_GRP = ("blk_0", "blk_1", "grp")
NEG = -1e30
LOWEST = -3e38
TO_LOG2 = HEAD_DIM**-0.5 * 1.4426950408889634


def kernel(
    G, NZ, NX, C,
    q_hbm, nk_hbm, nv_hbm, ck, cv, hits_hbm, counts_hbm, assign_hbm,
    out,
    hits, counts, assign, q2, nk2, nv2, wide, q3, kvf, kv3, Q, KA, V, VT, kvn, S0, S1, M0, M1,
    SB, RB, SL, RL, res, out3, size,
    loc, sent_sem, q_sem, n_sem, cache_sem, ring_sem, part_sem, o_sem,
):
    g, z, x = lax.axis_index("grp"), lax.axis_index("blk_0"), lax.axis_index("blk_1")
    T = NX * G
    GR = G * GROUP
    HX = NX // 2
    HR = HX * GR
    N1 = NX * C
    NK = KA.shape[0]
    PN = NK - N1
    HEADS = NX * GROUP
    Y = G // 2
    H = NZ // 2
    f32, bf = jnp.float32, jnp.bfloat16

    def remote(src, dst, ssem, rsem, **where):
        return pltpu.make_async_remote_copy(
            src_ref=src, dst_ref=dst, send_sem=ssem, recv_sem=rsem,
            device_id=where, device_id_type=pl.DeviceIdType.MESH,
        )

    def loop(start, n, fn):
        def body(i, carry):
            fn(i)
            return carry
        lax.fori_loop(start, n, body, 0)

    def peer(i):
        k = i // 2
        far = Y // 2 if k == 0 else (Y - k) // 2
        step = far if k % 2 == 1 else Y - far
        return lax.rem(g // 2 + step, Y) * 2 + lax.rem(g + 1 + i, 2)

    turns = [lax.rem(x + 1 + j, NX) for j in range(NX)]

    peers = [peer(i) for i in range(G - 1)]

    def others(fn):
        for p in peers:
            for t in turns:
                fn(p, t)
        for t in turns[:-1]:
            fn(g, t)

    barrier = pltpu.get_barrier_semaphore()

    def greet(**where):
        pl.semaphore_signal(barrier, 1, device_id=where, device_id_type=pl.DeviceIdType.MESH)

    others(lambda p, t: greet(grp=p, blk_1=t))
    after, before = lax.rem(z + 1, NZ), lax.rem(z + NZ - 1, NZ)
    greet(blk_0=after)
    greet(blk_0=before)
    greet(blk_0=lax.rem(z + 2, NZ))
    greet(blk_0=lax.rem(z + NZ - 2, NZ))

    own_lane = pl.ds(pl.multiple_of(x * HEAD_DIM, HEAD_DIM), HEAD_DIM)
    low = pl.ds(0, HEAD_DIM)

    def rows_from(p):
        return pl.ds(pl.multiple_of(p * C, C), C)

    ins = [
        pltpu.make_async_copy(q_hbm, q2, loc.at[0]),
        pltpu.make_async_copy(nk_hbm, nk2, loc.at[1]),
        pltpu.make_async_copy(nv_hbm, nv2, loc.at[2]),
        pltpu.make_async_copy(ck.at[:, own_lane], KA.at[rows_from(x), low], loc.at[3]),
        pltpu.make_async_copy(cv.at[:, own_lane], V.at[rows_from(x)], loc.at[4]),
        pltpu.make_async_copy(hits_hbm, hits, loc.at[5]),
        pltpu.make_async_copy(counts_hbm, counts, loc.at[6]),
        pltpu.make_async_copy(assign_hbm, assign, loc.at[7]),
    ]
    for c in ins:
        c.start()

    ins[0].wait()
    for h in range(HEADS):
        wide[pl.ds(h, G, stride=HEADS), :] = q2[:, h * HEAD_DIM : (h + 1) * HEAD_DIM].astype(f32)
    q3[...] = wide[...].astype(bf).reshape(G, NX, GROUP, HEAD_DIM)
    ins[1].wait()
    ins[2].wait()
    for h in range(NX):
        cut = slice(h * HEAD_DIM, (h + 1) * HEAD_DIM)
        kvf[pl.ds(2 * h, G, stride=2 * NX), :] = nk2[:, cut].astype(f32)
        kvf[pl.ds(2 * h + 1, G, stride=2 * NX), :] = nv2[:, cut].astype(f32)
    kv3[...] = kvf[...].reshape(G, NX, 2, HEAD_DIM).astype(bf)

    pl.semaphore_wait(barrier, G * NX - 1 + 4)

    def q_copy(p, t):
        return remote(q3.at[p, t], Q.at[z, x * G + g], sent_sem.at[0], q_sem.at[x], grp=p, blk_1=t)

    def n_copy(p, t):
        return remote(kv3.at[p, t], kvn.at[x * G + g], sent_sem.at[1], n_sem.at[0], grp=p, blk_1=t)

    def landed(ref, sem):
        pltpu.make_async_copy(ref, ref, sem).wait()

    def k_copy(i):
        p = lax.rem(x + i, NX)
        lane = pl.ds(pl.multiple_of(p * HEAD_DIM, HEAD_DIM), HEAD_DIM)
        return remote(ck.at[:, lane], KA.at[rows_from(x), low], sent_sem.at[2], cache_sem.at[0], blk_1=p)

    def v_copy(i):
        p = lax.rem(x + i, NX)
        lane = pl.ds(pl.multiple_of(p * HEAD_DIM, HEAD_DIM), HEAD_DIM)
        return remote(cv.at[:, lane], V.at[rows_from(x)], sent_sem.at[2], cache_sem.at[1], blk_1=p)

    others(lambda p, t: q_copy(p, t).start())
    loop(1, NX, lambda i: k_copy(i).start())
    others(lambda p, t: n_copy(p, t).start())
    loop(1, NX, lambda i: v_copy(i).start())

    Q[z, x * G + g] = q3[g, x]
    kvn[x * G + g] = kv3[g, x]

    for c in ins[5:]:
        c.wait()
    limit = hits[0] - z * N1
    row = lax.broadcasted_iota(jnp.int32, (NK, HEAD_DIM), 0)
    lane0 = lax.broadcasted_iota(jnp.int32, (NK, HEAD_DIM), 1) == 0
    barred = lane0 & (row >= limit) & (row < N1)
    KA[:, HEAD_DIM:] = jnp.where(barred, NEG, 0.0).astype(bf)
    KA[N1:, 0:HEAD_DIM] = jnp.zeros((PN, HEAD_DIM), bf)
    V[N1:, :] = jnp.zeros((PN, HEAD_DIM), bf)
    VT[HEAD_DIM:, :] = jnp.ones((ONES, NK), bf)
    for way in (0, 1):
        for s in range(HX):
            RB[way, NZ + 1, s] = jnp.zeros((HEAD_DIM, GR), bf)
            RL[way, NZ + 1, s] = jnp.full((1, GR), LOWEST, f32)

    def held(way, k):
        return lax.rem(z + (NZ - k if way == 0 else k), NZ)

    def go(way):
        return after if way == 0 else before

    def q_rows(way, k, s):
        return Q.at[held(way, k), pl.ds((way * HX + s) * G, G)]

    routes = {0: (2, 1), 2: (4, 3), 4: (5,), 5: (6,), 6: (7,)} if NZ == 8 else {0: (2, 1), 2: (3,)}
    due = {3: (3,), 5: (5,), 6: (6,), 1: (1,), 7: (7,)} if NZ == 8 else {1: (1,), 3: (3,)}

    def q_on(way, k, s, hop):
        ref = q_rows(way, k, s)
        to = lax.rem(z + (hop if way == 0 else NZ - hop), NZ)
        return remote(ref, ref, sent_sem.at[3], ring_sem.at[way, k + hop - 1, s], blk_0=to)

    for s in range(HX):
        for way in (0, 1):
            t = way * HX + s

            @pl.when(x == t)
            def _():
                landed(Q.at[z, pl.ds(t * G, G - 1)], q_sem.at[t])

            @pl.when(x != t)
            def _():
                landed(Q.at[z, pl.ds(t * G, G)], q_sem.at[t])

            q_on(way, 0, s, 2).start()

    def pass_on(k):
        for s in range(HX):
            for way in (0, 1):
                landed(q_rows(way, k, s), ring_sem.at[way, k - 1, s])
                for further in routes.get(k, ())[:1]:
                    q_on(way, k, s, further - k).start()
        for further in routes.get(k, ())[1:]:
            for s in range(HX):
                for way in (0, 1):
                    q_on(way, k, s, further - k).start()

    for k in range(2, H, 2):
        pass_on(k)
    for s in range(HX):
        for way in (0, 1):
            q_on(way, 0, s, 1).start()

    landed(kvn.at[pl.ds(0, T - 1)], n_sem.at[0])
    KA[N1 : N1 + T, 0:HEAD_DIM] = kvn[:, 0, :]
    V[N1 : N1 + T, :] = kvn[:, 1, :]
    ins[3].wait()
    landed(V.at[pl.ds(0, (NX - 1) * C)], cache_sem.at[0])

    def position(token, block):
        pos = jnp.full(token.shape, 1 << 20, jnp.int32)
        for s in range(NX):
            here = (token >= s * G) & (token < (s + 1) * G)
            pos = jnp.where(here, assign[block * NX + s] * G + (token - s * G), pos)
        return pos

    first = (lax.broadcasted_iota(jnp.int32, (HR, HEAD_DIM), 1) == 0).astype(f32).astype(bf)

    def scores(k, way, S, M):
        c = held(way, k)
        q = Q[c, pl.ds(way * HX * G, HX * G)].reshape(HR, HEAD_DIM)
        q = jnp.concatenate([q, first], axis=1)
        s = lax.dot_general(KA[...], q, (((1,), (1,)), ((), ())), preferred_element_type=f32)
        pt = position(way * HX * G + lax.broadcasted_iota(jnp.int32, (1, HR), 1) // GROUP, c)
        pu = position(lax.broadcasted_iota(jnp.int32, (PN, 1), 0), z)
        old, new = s[:N1], jnp.where(pu <= pt, s[N1:], NEG)
        S[0:N1] = old
        S[N1:] = new
        M[...] = jnp.maximum(
            jnp.max(old.reshape(N1 // 8, 8, HR), axis=0), jnp.max(new.reshape(PN // 8, 8, HR), axis=0)
        )

    def part_on(way, k, s):
        slot = jnp.where(k >= H, k + 1, k - 1)
        to = jnp.where(k >= H, go(way), go(1 - way))
        return (
            remote(SB.at[way, k, s], RB.at[way, slot, s], sent_sem.at[4], part_sem.at[way, slot, s], blk_0=to),
            remote(SL.at[way, k, s], RL.at[way, slot, s], sent_sem.at[5], part_sem.at[way, slot, s], blk_0=to),
        )

    def part_in(way, slot, s):
        landed(size, part_sem.at[way, slot, s])

    def blend(k, way, S, M):
        top = jnp.max(M[...], axis=0, keepdims=True)
        p = jnp.exp2((S[...] - top) * TO_LOG2).astype(bf)
        both = jnp.dot(VT[:, :N1], p[:N1], preferred_element_type=f32)
        both = both + jnp.dot(VT[:, N1:], p[N1:], preferred_element_type=f32)
        weight = both[HEAD_DIM : HEAD_DIM + 1]
        level = top * TO_LOG2 + jnp.log2(weight)
        inverse = 1.0 / weight
        fresh = (k == 0) | (k == H - 1) | (k == H)
        slot = jnp.where(fresh, NZ + 1, k)
        for s in range(HX):
            cut = slice(s * GR, (s + 1) * GR)

            @pl.when(jnp.logical_not(fresh))
            def _():
                part_in(way, k, s)

            there, here = RL[way, slot, s], level[:, cut]
            high = jnp.maximum(there, here)
            a, b = jnp.exp2(there - high), jnp.exp2(here - high)
            both_parts = a + b
            a, b = a / both_parts, b / both_parts * inverse[:, cut]
            merged = RB[way, slot, s].astype(f32) * a + both[:HEAD_DIM, cut] * b
            SB[way, k, s] = merged.astype(bf)
            SL[way, k, s] = high + jnp.log2(both_parts)

            @pl.when(k > 0)
            def _():
                for copy in part_on(way, k, s):
                    copy.start()

    pass_on(H)
    scores(H, 0, S0, M0)
    ins[4].wait()
    landed(V.at[pl.ds(0, (NX - 1) * C)], cache_sem.at[1])
    VT[0:HEAD_DIM, :] = V[...].T

    def step_of(n):
        return jnp.where(lax.rem(n, 2) == 0, H + n // 2, H - 1 - n // 2)

    def turn(n):
        k, m = step_of(n), step_of(jnp.minimum(n + 1, NZ - 1))
        scores(k, 1, S1, M1)
        blend(k, 0, S0, M0)
        for at, steps in due.items():

            @pl.when((m == at) & (n < NZ - 1))
            def _():
                for step in steps:
                    pass_on(step)

        scores(m, 0, S0, M0)
        blend(k, 1, S1, M1)

    loop(0, NZ, turn)

    def o_copy(p, t):
        return remote(res.at[t * G + p], out3.at[g, x], sent_sem.at[6], o_sem.at[0], grp=p, blk_1=t)

    for s in range(HX):
        for way in (0, 1):
            t = way * HX + s
            part_in(way, 0, s)
            part_in(way, NZ, s)
            one, two, own = RL[way, 0, s], RL[way, NZ, s], SL[way, 0, s]
            high = jnp.maximum(jnp.maximum(one, two), own)
            a, b, c = jnp.exp2(one - high), jnp.exp2(two - high), jnp.exp2(own - high)
            done = RB[way, 0, s].astype(f32) * a + RB[way, NZ, s].astype(f32) * b
            done = (done + SB[way, 0, s].astype(f32) * c) / (a + b + c)
            done = done.T
            place = assign[z * NX + t] * G + lax.broadcasted_iota(jnp.int32, (GR, 1), 0) // GROUP
            done = jnp.where(place < counts[0], done, 0.0).astype(bf)
            res[t * G : (t + 1) * G] = done.reshape(G, GROUP, HEAD_DIM)

            for p in peers:
                o_copy(p, t).start()
            pl.when(x != t)(lambda t=t: o_copy(g, t).start())
    out3[g, x] = res[x * G + g]
    landed(res.at[pl.ds(0, T - 1)], o_sem.at[0])
    wide[...] = out3[...].reshape(G * HEADS, HEAD_DIM).astype(f32)
    for h in range(HEADS):
        out[:, h * HEAD_DIM : (h + 1) * HEAD_DIM] = wide[pl.ds(h, G, stride=HEADS), :].astype(bf)

    landed(res.at[pl.ds(0, T - 1)], sent_sem.at[0])
    landed(kvn.at[pl.ds(0, T - 1)], sent_sem.at[1])
    landed(KA.at[pl.ds(0, (NX - 1) * C)], sent_sem.at[2])
    landed(Q.at[pl.ds(0, NZ - 1), pl.ds(0, 2 * HX * G)], sent_sem.at[3])
    landed(SB.at[:, pl.ds(1, NZ - 1)], sent_sem.at[4])
    landed(SL.at[:, pl.ds(1, NZ - 1)], sent_sem.at[5])
    landed(res.at[pl.ds(0, T - 1)], sent_sem.at[6])


def local(queries, cache_keys, cache_values, new_keys, new_values, hits, counts, assign):
    NZ, NX, G = lax.axis_size("blk_0"), lax.axis_size("blk_1"), lax.axis_size("grp")
    C = cache_keys.shape[1]
    T = NX * G
    GR = G * GROUP
    HX = NX // 2
    HR = HX * GR
    N1 = NX * C
    NK = N1 + max(T, 128)
    W = NX * GROUP * HEAD_DIM
    hbm = pl.BlockSpec(memory_space=pltpu.HBM)
    bf, f32 = jnp.bfloat16, jnp.float32
    dma = pltpu.SemaphoreType.DMA
    held = (
        queries.reshape(G, W), new_keys.reshape(G, NX * HEAD_DIM), new_values.reshape(G, NX * HEAD_DIM),
        cache_keys[0], cache_values[0],
    )
    made = pl.pallas_call(
        functools.partial(kernel, G, NZ, NX, C),
        out_shape=jax.ShapeDtypeStruct((G, W), bf),
        in_specs=[hbm] * 8,
        out_specs=pl.BlockSpec(memory_space=pltpu.VMEM),
        scratch_shapes=[
            pltpu.SMEM((1,), jnp.int32),
            pltpu.SMEM((1,), jnp.int32),
            pltpu.SMEM((NZ * NX,), jnp.int32),
            pltpu.VMEM((G, W), bf),
            pltpu.VMEM((G, NX * HEAD_DIM), bf),
            pltpu.VMEM((G, NX * HEAD_DIM), bf),
            pltpu.VMEM((G * NX * GROUP, HEAD_DIM), f32),
            pltpu.VMEM((G, NX, GROUP, HEAD_DIM), bf),
            pltpu.VMEM((G * NX * 2, HEAD_DIM), f32),
            pltpu.VMEM((G, NX, 2, HEAD_DIM), bf),
            pltpu.VMEM((NZ, T, GROUP, HEAD_DIM), bf),
            pltpu.VMEM((NK, 2 * HEAD_DIM), bf),
            pltpu.VMEM((NK, HEAD_DIM), bf),
            pltpu.VMEM((HEAD_DIM + ONES, NK), bf),
            pltpu.VMEM((T, 2, HEAD_DIM), bf),
            pltpu.VMEM((NK, HR), f32),
            pltpu.VMEM((NK, HR), f32),
            pltpu.VMEM((8, HR), f32),
            pltpu.VMEM((8, HR), f32),
            pltpu.VMEM((2, NZ, HX, HEAD_DIM, GR), bf),
            pltpu.VMEM((2, NZ + 2, HX, HEAD_DIM, GR), bf),
            pltpu.VMEM((2, NZ, HX, 1, GR), f32),
            pltpu.VMEM((2, NZ + 2, HX, 1, GR), f32),
            pltpu.VMEM((T, GROUP, HEAD_DIM), bf),
            pltpu.VMEM((G, NX, GROUP, HEAD_DIM), bf),
            pltpu.VMEM((HEAD_DIM // 2 + 1, 1, GR), f32),
            dma((8,)), dma((7,)), dma((NX,)), dma((1,)), dma((2,)),
            dma((2, NZ - 1, HX)), dma((2, NZ + 1, HX)), dma((1,)),
        ],
        compiler_params=pltpu.CompilerParams(
            collective_id=0, has_side_effects=True, vmem_limit_bytes=48 * 1024 * 1024
        ),
        name="attend",
    )(
        *(pltpu.with_memory_space_constraint(a, pltpu.HBM) for a in held), hits, counts,
        pltpu.with_memory_space_constraint(assign[0], pltpu.HBM),
    )
    return made.reshape(G, 1, W)


def solution(mesh):
    finer = Mesh(mesh.devices.reshape(mesh.shape["grp"], 8, 4), ("grp", "blk_0", "blk_1"))
    in_specs = (
        P(None, BLK_GRP, None),
        P("grp", BLK, None),
        P("grp", BLK, None),
        P(None, BLK_GRP, None),
        P(None, BLK_GRP, None),
        P("grp"),
        P("grp"),
        P("grp", None),
    )
    out_specs = P(None, BLK_GRP, None)
    return jax.shard_map(local, mesh=finer, in_specs=in_specs, out_specs=out_specs, check_vma=False)
```
